512 devices in a mesh: grp: 8 (over x, z_hi), seq: 64 (over y, z_lo, core).
Axes of the slice: x: 4, y: 4, z: 16 (z_hi: 2, z_lo: 8; z = z_hi * 8 + z_lo), core: 2. Of those that a mesh axis runs over, the one named last changes fastest.
Arguments:
- queries: bfloat16 [512, 5120], P(('grp', 'seq')), may hold values from -10 to 10
- query_tangent: bfloat16 [512, 5120], P(('grp', 'seq')), may hold values from -6 to 6
- keys: bfloat16 [32768, 5120], P('seq', 'grp'), may hold values from -10 to 10
- key_tangent: bfloat16 [32768, 5120], P('seq', 'grp'), may hold values from -6 to 6
- values: bfloat16 [32768, 5120], P('seq', 'grp'), may hold values from -6 to 6
- value_tangent: bfloat16 [32768, 5120], P('seq', 'grp'), may hold values from -6 to 6
Outputs:
- attended: bfloat16 [512, 5120], P(('grp', 'seq'))
- attended_tangent: bfloat16 [512, 5120], P(('grp', 'seq'))
The draws below stay inside these ranges and needn't reach their ends.
All inputs are finite; a program needn't handle non-finite values.
Results may differ from the reference program's by a relative error of at most 0.0084.
Values may be sent and summed in bfloat16 or wider, within the bound.
A program may use at most 64 MiB of HBM per device.

```python
import jax
import jax.numpy as jnp
from jax import lax

HEAD_DIM = 128
KEYS_DEV = 512
HEADS = 40
SEQ = 32768
Q_SLAB = 512
N_SEQ = 64


def draw_keys(key, part):
    drawn = jnp.clip(1.7 * jax.random.normal(jax.random.fold_in(key, 11), (SEQ, HEADS * HEAD_DIM), jnp.float32), -10.0, 10.0)
    return drawn.astype(jnp.bfloat16)


def draw_queries(key, part):
    drawn = jnp.clip(1.7 * jax.random.normal(jax.random.fold_in(key, 13), (Q_SLAB, HEADS * HEAD_DIM), jnp.float32), -10.0, 10.0)
    return drawn.astype(jnp.bfloat16)


def level_of(stream_key, extent, shards, low, top_value):
    level = 1.0
    for axis_at, blocks in shards:
        draws = jax.random.uniform(jax.random.fold_in(jax.random.fold_in(stream_key, 6), axis_at), (blocks,), jnp.float32, low / len(shards), top_value / len(shards))
        level = level * jnp.repeat(jnp.exp(draws), extent[axis_at] // blocks).reshape((-1,) + (1,) * (len(extent) - 1 - axis_at))
    return level


def bell_draw(own_key, extent, scale, limit, cuts=(), kind=jnp.bfloat16):
    entries = scale * jax.random.normal(own_key, extent, jnp.float32)
    if cuts:
        entries = entries * level_of(own_key, extent, cuts, -0.22, 0.18)
    return jnp.clip(entries, -limit, limit).astype(kind)


def setup_inputs(seed: int = 0) -> dict:
    seeds = jax.random.split(jax.random.key(seed), 7)
    return {
        "queries": draw_queries(jax.random.fold_in(seeds[6], 71), 0),
        "query_tangent": bell_draw(seeds[1], (Q_SLAB, HEADS * HEAD_DIM), 1.0, 6.0, ((0, 512),)),
        "keys": draw_keys(jax.random.fold_in(seeds[6], 71), 0),
        "key_tangent": bell_draw(seeds[3], (SEQ, HEADS * HEAD_DIM), 1.0, 6.0, ((0, 64), (1, 8))),
        "values": bell_draw(seeds[4], (SEQ, HEADS * HEAD_DIM), 1.0, 6.0, ((0, 64), (1, 8))),
        "value_tangent": bell_draw(seeds[5], (SEQ, HEADS * HEAD_DIM), 1.0, 6.0, ((0, 64), (1, 8))),
    }


def split_heads(matrix):
    return matrix.reshape(matrix.shape[0], HEADS, HEAD_DIM).transpose(1, 0, 2)


def one_head(operands):
    query, q_tan, key, k_tan, value, v_tan = [m.astype(jnp.float32) for m in operands]
    scale = HEAD_DIM ** -0.5
    logit_scores = jnp.dot(query, key.T, preferred_element_type=jnp.float32) * scale
    tangent_scores = (jnp.dot(q_tan, key.T, preferred_element_type=jnp.float32) + jnp.dot(query, k_tan.T, preferred_element_type=jnp.float32)) * scale
    score_blocks = logit_scores.reshape(Q_SLAB, N_SEQ, KEYS_DEV)
    tangent_blocks = tangent_scores.reshape(Q_SLAB, N_SEQ, KEYS_DEV)
    block_max = jnp.max(score_blocks, axis=2, keepdims=True)
    weights = jnp.exp(score_blocks - block_max)
    mixed = weights * tangent_blocks
    block_total = jnp.sum(weights, axis=2, keepdims=True)
    block_denominator_tangent = jnp.sum(mixed, axis=2, keepdims=True)
    weights_reduced_precision = weights.astype(jnp.bfloat16).astype(jnp.float32)
    mixed_reduced_precision = mixed.astype(jnp.bfloat16).astype(jnp.float32)
    value_block_list = value.reshape(N_SEQ, KEYS_DEV, HEAD_DIM)
    value_tangent_block_list = v_tan.reshape(N_SEQ, KEYS_DEV, HEAD_DIM)
    block_numerator = jnp.einsum("jtx,txh->jth", weights_reduced_precision, value_block_list)
    block_numerator_tangent = jnp.einsum("jtx,txh->jth", weights_reduced_precision, value_tangent_block_list) + jnp.einsum("jtx,txh->jth", mixed_reduced_precision, value_block_list)
    row_max = jnp.max(block_max, axis=1, keepdims=True)
    factor = jnp.exp(block_max - row_max)
    numer = jnp.sum(factor * block_numerator, axis=1)
    numer_tangent = jnp.sum(factor * block_numerator_tangent, axis=1)
    total = jnp.sum(factor * block_total, axis=1)
    total_tangent = jnp.sum(factor * block_denominator_tangent, axis=1)
    output = numer / total
    out_tangent = (numer_tangent - output * total_tangent) / total
    return output, out_tangent


def reference(queries, query_tangent, keys, key_tangent, values, value_tangent):
    stacked = tuple(split_heads(m) for m in (queries, query_tangent, keys, key_tangent, values, value_tangent))
    output, out_tangent = lax.map(one_head, stacked)
    attended = output.transpose(1, 0, 2).reshape(Q_SLAB, HEADS * HEAD_DIM).astype(jnp.bfloat16)
    attended_tangent = out_tangent.transpose(1, 0, 2).reshape(Q_SLAB, HEADS * HEAD_DIM).astype(jnp.bfloat16)
    return attended, attended_tangent
```

```python
import functools

import jax
import jax.numpy as jnp
from jax import lax
from jax.experimental import pallas as pl
from jax.experimental.pallas import tpu as pltpu
from jax.sharding import PartitionSpec as P

HEAD_DIM = 128
X, Y, ZH, ZL = 4, 4, 2, 8
Z = ZH * ZL
GRP = X * ZH
B = 2 * X
MESH = pl.DeviceIdType.MESH
F32, BF16 = jnp.float32, jnp.bfloat16


def merge(planes, heads):
    count = planes.count
    stats = [planes(i, 2 * heads) for i in range(count)]
    axis = stats[0].ndim - 1
    stats = [s + pltpu.roll(s, 128 - 2 * heads, axis) + pltpu.roll(s, 128 - 4 * heads, axis) for s in stats]
    top = functools.reduce(jnp.maximum, stats)
    grown = [jnp.exp(s - top) for s in stats]
    whole = sum(grown)
    weights = [g / whole for g in grown]
    moved = [pltpu.roll(w, heads, axis) for w in weights]
    score = sum(w * s for w, s in zip(moved, stats))
    tilts = [w * (s - score) for w, s in zip(moved, stats)]
    lane = lax.broadcasted_iota(jnp.int32, top.shape, axis)
    merged = jnp.where(lane < heads, top + jnp.log(whole), score)
    outs, tans = [], []
    for h in range(heads):
        out = tan = None
        for i in range(count):
            w = weights[i][..., h : h + 1]
            c = tilts[i][..., heads + h : heads + h + 1]
            o, t = planes(i, h), planes(i, heads + h)
            a, b = w * o, w * t + c * o
            out, tan = (a, b) if i == 0 else (out + a, tan + b)
        outs.append(out)
        tans.append(tan)
    return outs, tans, merged


def pieces(stats, heads):
    axis = stats.ndim - 1
    lane = lax.broadcasted_iota(jnp.int32, stats.shape, axis)
    stats = jnp.where(lane < 2 * heads, stats, 0.0)
    high = stats.astype(BF16).astype(F32)
    rest = stats - high
    middle = rest.astype(BF16).astype(F32)
    low = (rest - middle).astype(BF16).astype(F32)
    return high + pltpu.roll(middle, 2 * heads, axis) + pltpu.roll(low, 4 * heads, axis)


class Planes:
    def __init__(self, refs):
        self.refs, self.count = refs, len(refs)

    def __call__(self, i, p):
        return self.refs[i][p].astype(F32)


def kernel(heads, q_in, t_in, k_hbm, kt_hbm, v_hbm, vt_hbm, o_out, t_out,
           kk, vv, stage, xrecv, zsend, qbuf, stat, mine, theirs, pair, yrecv, total, zrecv, final, orecv,
           load_sem, xs_sem, xr_sem, zs_sem, zr_sem, fs_sem, fr_sem, ys_sem, yr_sem,
           ps_sem, pr_sem, rs_sem, rr_sem, cs_sem, cr_sem, es_sem, er_sem):
    grp, seq = lax.axis_index("grp"), lax.axis_index("seq")
    x, zh = lax.div(grp, ZH), lax.rem(grp, ZH)
    y, zl, core = lax.div(seq, 2 * ZL), lax.rem(lax.div(seq, 2), ZL), lax.rem(seq, 2)
    z = zh * ZL + zl
    other = 1 - core

    def device(x_, y_, z_, core_):
        return (x_ * ZH + lax.div(z_, ZL), (y_ * ZL + lax.rem(z_, ZL)) * 2 + core_)

    def remote(src, dst, send, recv, where):
        return pltpu.make_async_remote_copy(src_ref=src, dst_ref=dst, send_sem=send, recv_sem=recv,
                                            device_id=where, device_id_type=MESH)

    here = (grp, seq)
    partner = (grp, seq + 1 - 2 * core)
    planes = 2 * heads + 1

    barrier = pltpu.get_barrier_semaphore()

    def greet(where):
        pl.semaphore_signal(barrier, inc=1, device_id=where, device_id_type=MESH)

    for k in range(1, Z):
        greet(device(x, y, lax.rem(z + k, Z), core))

    @pl.when(core != zh)
    def _():
        for i in range(ZL):
            greet(device(x, y, core * ZL + i, zh))

    for d in range(1, Y):
        greet(device(x, lax.rem(y + d, Y), z, core))
    for d in range(X):
        if d:
            greet(device(lax.rem(x + d, X), y, z, core))
        greet(device(lax.rem(x + d, X), y, z, other))

    loads = []
    for h in range(heads):
        cols = pl.ds(h * HEAD_DIM, HEAD_DIM)
        loads += [
            pltpu.make_async_copy(k_hbm.at[:, cols], kk.at[h, :, pl.ds(0, HEAD_DIM)], load_sem.at[h, 0]),
            pltpu.make_async_copy(kt_hbm.at[:, cols], kk.at[h, :, pl.ds(HEAD_DIM, HEAD_DIM)], load_sem.at[h, 1]),
            pltpu.make_async_copy(v_hbm.at[:, cols], vv.at[h, :, pl.ds(0, HEAD_DIM)], load_sem.at[h, 2]),
            pltpu.make_async_copy(vt_hbm.at[:, cols], vv.at[h, :, pl.ds(HEAD_DIM, HEAD_DIM)], load_sem.at[h, 3]),
        ]
    for copy in loads:
        copy.start()

    for p, ref in enumerate((q_in, t_in)):
        for g in range(GRP):
            for h in range(heads):
                at = (g * heads + h) * HEAD_DIM
                stage[p, g, h : h + 1, :] = ref[0:1, at : at + HEAD_DIM].astype(F32)

    pl.semaphore_wait(barrier, (Z - 1) + (Y - 1) + (2 * X - 1) + jnp.where(core != zh, ZL, 0))

    row = x * 2 + core

    def x_copy(x_, p):
        return remote(stage.at[p, pl.ds(x_ * ZH, ZH)], xrecv.at[row], xs_sem.at[x_, p], xr_sem.at[row],
                      device(x_, y, z, p))

    for d in range(X):
        x_ = lax.rem(x + d, X)
        if d:
            x_copy(x_, core).start()
        x_copy(x_, other).start()
    xrecv[row] = stage[core, pl.ds(x * ZH, ZH)]
    for d in range(X):
        x_ = lax.rem(x + d, X)
        for c in ([other] if d == 0 else [core, other]):
            slot = x_ * 2 + c
            remote(stage.at[0, pl.ds(0, ZH)], xrecv.at[slot], xs_sem.at[0, 0], xr_sem.at[slot], here).wait_recv()
    for g in range(ZH):
        for h in range(heads):
            zsend[g, h] = xrecv[:, g, h, :].astype(BF16)

    def z_copy(z_):
        return remote(zsend.at[lax.div(z_, ZL)], qbuf.at[core, y, z], zs_sem.at[z_], zr_sem.at[z],
                      device(x, y, z_, core))

    order = []
    for k in range(1, Z // 2 + 1):
        order += [k] if 2 * k == Z else [k, Z - k]
    for k in reversed(order):
        z_copy(lax.rem(z + k, Z)).start()
    qbuf[core, y, z] = zsend[zh]

    def y_copy(z_, d):
        y_ = lax.rem(y + d, Y)
        return remote(qbuf.at[core, y, z_], qbuf.at[core, y, z_], ys_sem.at[d, z_], yr_sem.at[y],
                      device(x, y_, z, core))

    def own_copy(z_):
        return remote(qbuf.at[core, y, z_], qbuf.at[core, y, z_], fs_sem.at[y, z_], fr_sem.at[y], partner)

    def forward(z_):
        for d in (2, 1, 3):
            if d < Y:
                y_copy(z_, d).start()
        own_copy(z_).start()

    forward(z)

    def z_step(j, carry):
        half = lax.div(j + 1, 2)
        k = jnp.where(lax.rem(j, 2) == 1, half, Z - half)
        z_ = lax.rem(z + k, Z)
        remote(zsend.at[0], qbuf.at[core, y, z_], zs_sem.at[0], zr_sem.at[z_], here).wait_recv()
        forward(z_)
        return carry

    lax.fori_loop(1, Z, z_step, 0)

    def block_copy(y_):
        return remote(qbuf.at[core, y_], qbuf.at[core, y_], fs_sem.at[y_, 0], fr_sem.at[y_], partner)

    def take(y_):
        remote(qbuf.at[core, y_], qbuf.at[core, y_], ys_sem.at[0, 0], yr_sem.at[y_], here).wait_recv()
        block_copy(y_).start()

    def ready(y_):
        remote(qbuf.at[other, y_], qbuf.at[other, y_], fs_sem.at[0, 0], fr_sem.at[y_], here).wait_recv()

    rows = Z * B
    scale = HEAD_DIM ** -0.5

    def attend(y_):
        def one_head(h, carry):
            q = qbuf[0, y_, :, h].astype(F32).reshape(rows, HEAD_DIM).astype(BF16)
            t = qbuf[1, y_, :, h].astype(F32).reshape(rows, HEAD_DIM).astype(BF16)
            left = jnp.concatenate(
                [jnp.concatenate([q, jnp.zeros_like(q)], axis=1), jnp.concatenate([t, q], axis=1)], axis=0)
            both = lax.dot_general(left, kk[h], (((1,), (1,)), ((), ())), preferred_element_type=F32)
            scores, tangents = both[:rows] * scale, both[rows:] * scale
            top = jnp.max(scores, axis=1, keepdims=True)
            weights = jnp.exp(scores - top)
            mixed = weights * tangents
            whole = jnp.sum(weights, axis=1, keepdims=True)
            whole_t = jnp.sum(mixed, axis=1, keepdims=True)
            low = jnp.concatenate([weights.astype(BF16), mixed.astype(BF16)], axis=0)
            sums = lax.dot_general(low, vv[h], (((1,), (0,)), ((), ())), preferred_element_type=F32)
            numer = sums[:rows, :HEAD_DIM]
            numer_t = sums[:rows, HEAD_DIM:] + sums[rows:, :HEAD_DIM]
            out = numer / whole
            score = whole_t / whole
            tan = numer_t / whole - out * score
            mine[y_, :, h] = out.reshape(Z, B, HEAD_DIM).astype(BF16)
            mine[y_, :, heads + h] = tan.reshape(Z, B, HEAD_DIM).astype(BF16)
            lane = lax.broadcasted_iota(jnp.int32, (rows, 128), 1)
            stat[...] = jnp.where(lane == h, top + jnp.log(whole), jnp.where(lane == heads + h, score, stat[...]))
            return carry

        lax.fori_loop(0, heads, one_head, 0)
        mine[y_, :, 2 * heads] = pieces(stat[...], heads).reshape(Z, B, 128).astype(BF16)
        part_copy(y_).start()

    def part_copy(y_):
        return remote(mine.at[y_, pl.ds(other * ZL, ZL)], theirs.at[y_], ps_sem.at[y_], pr_sem.at[y_], partner)

    def join(y_):
        remote(theirs.at[y_], theirs.at[y_], ps_sem.at[0], pr_sem.at[y_], here).wait_recv()

        def step(i, carry):
            parts = Planes([mine.at[y_, core * ZL + i], theirs.at[y_, i]])
            outs, tans, merged = merge(parts, heads)
            for h in range(heads):
                pair[y_, i, h] = outs[h].astype(BF16)
                pair[y_, i, heads + h] = tans[h].astype(BF16)
            pair[y_, i, 2 * heads] = pieces(merged, heads).astype(BF16)
            return carry

        lax.fori_loop(0, ZL, step, 0)

    def row_copy(d):
        y_ = lax.rem(y + d, Y)
        return remote(pair.at[y_], yrecv.at[y], rs_sem.at[d], rr_sem.at[y], device(x, y_, z, core))

    turn = [d for d in (1, 3, 2) if d < Y]
    ys = [lax.rem(y + d, Y) for d in turn]

    stat[...] = jnp.zeros_like(stat)
    for copy in loads:
        copy.wait()
    ready(y)
    attend(y)
    take(ys[0])
    if len(ys) > 1:
        take(ys[1])
    for i, d in enumerate(turn):
        ready(ys[i])
        attend(ys[i])
        if i + 2 < len(ys):
            take(ys[i + 2])
        if i:
            join(ys[i - 1])
            row_copy(turn[i - 1]).start()
    join(ys[-1])
    row_copy(turn[-1]).start()
    join(y)
    for y_ in ys:
        remote(pair.at[0], yrecv.at[y_], rs_sem.at[0], rr_sem.at[y_], here).wait_recv()

    def z_target(i):
        return core * ZL + i

    def c_copy(i):
        return remote(total.at[i], zrecv.at[zl], cs_sem.at[i], cr_sem.at[zl], device(x, y, z_target(i), zh))

    def y_sum(i, carry):
        parts = Planes([pair.at[y, i]] + [yrecv.at[y_, i] for y_ in ys])
        outs, tans, merged = merge(parts, heads)
        for h in range(heads):
            total[i, h] = outs[h].astype(BF16)
            total[i, heads + h] = tans[h].astype(BF16)
        total[i, 2 * heads] = pieces(merged, heads).astype(BF16)

        @pl.when(z_target(i) != z)
        def _():
            c_copy(i).start()

        @pl.when(z_target(i) == z)
        def _():
            zrecv[zl] = total[i]

        return carry

    lax.fori_loop(0, ZL, y_sum, 0)

    def c_wait(i, carry):
        @pl.when(z_target(i) != z)
        def _():
            remote(total.at[0], zrecv.at[i], cs_sem.at[0], cr_sem.at[i], here).wait_recv()

        return carry

    lax.fori_loop(0, ZL, c_wait, 0)
    outs, tans, _ = merge(Planes([zrecv.at[i] for i in range(ZL)]), heads)
    for h in range(heads):
        final[:, 0, h, :] = outs[h]
        final[:, 1, h, :] = tans[h]

    group = x * ZH + core

    def e_copy(x_, c):
        return remote(final.at[x_ * 2 + c], orecv.at[group], es_sem.at[x_ * 2 + c], er_sem.at[group],
                      device(x_, y, z, c))

    for d in range(X):
        x_ = lax.rem(x + d, X)
        if d:
            e_copy(x_, core).start()
        e_copy(x_, other).start()
    orecv[group] = final[row]
    for d in range(X):
        x_ = lax.rem(x + d, X)
        for c in ([other] if d == 0 else [core, other]):
            slot = x_ * ZH + c
            remote(final.at[0], orecv.at[slot], es_sem.at[0], er_sem.at[slot], here).wait_recv()
    for p, ref in enumerate((o_out, t_out)):
        for g in range(GRP):
            for h in range(heads):
                at = (g * heads + h) * HEAD_DIM
                ref[0:1, at : at + HEAD_DIM] = orecv[g, p, h : h + 1, :].astype(BF16)

    for d in range(X):
        x_ = lax.rem(x + d, X)
        for c in ([other] if d == 0 else [core, other]):
            x_copy(x_, c).wait_send()
            e_copy(x_, c).wait_send()

    def sent(j, carry):
        z_ = lax.rem(z + j, Z)

        @pl.when(j > 0)
        def _():
            z_copy(z_).wait_send()

        for d in range(1, Y):
            y_copy(z_, d).wait_send()
        own_copy(z_).wait_send()
        return carry

    lax.fori_loop(0, Z, sent, 0)
    for d, y_ in zip(turn, ys):
        block_copy(y_).wait_send()
        part_copy(y_).wait_send()
        row_copy(d).wait_send()
    part_copy(y).wait_send()

    def c_sent(i, carry):
        @pl.when(z_target(i) != z)
        def _():
            c_copy(i).wait_send()

        return carry

    lax.fori_loop(0, ZL, c_sent, 0)


def per_device(queries, query_tangent, keys, key_tangent, values, value_tangent):
    count, width = keys.shape
    heads = width // HEAD_DIM
    planes = 2 * heads + 1
    pad = -(-heads // 8) * 8
    vmem, anywhere = pl.BlockSpec(memory_space=pltpu.VMEM), pl.BlockSpec(memory_space=pl.ANY)
    dma = pltpu.SemaphoreType.DMA
    return pl.pallas_call(
        functools.partial(kernel, heads),
        out_shape=(jax.ShapeDtypeStruct(queries.shape, BF16), jax.ShapeDtypeStruct(queries.shape, BF16)),
        in_specs=[vmem, vmem] + [anywhere] * 4,
        out_specs=(vmem, vmem),
        scratch_shapes=[
            pltpu.VMEM((heads, count, 2 * HEAD_DIM), BF16),
            pltpu.VMEM((heads, count, 2 * HEAD_DIM), BF16),
            pltpu.VMEM((2, GRP, pad, HEAD_DIM), F32),
            pltpu.VMEM((B, ZH, pad, HEAD_DIM), F32),
            pltpu.VMEM((ZH, heads, B, HEAD_DIM), BF16),
            pltpu.VMEM((2, Y, Z, heads, B, HEAD_DIM), BF16),
            pltpu.VMEM((Z * B, 128), F32),
            pltpu.VMEM((Y, Z, planes, B, HEAD_DIM), BF16),
            pltpu.VMEM((Y, ZL, planes, B, HEAD_DIM), BF16),
            pltpu.VMEM((Y, ZL, planes, B, HEAD_DIM), BF16),
            pltpu.VMEM((Y, ZL, planes, B, HEAD_DIM), BF16),
            pltpu.VMEM((ZL, planes, B, HEAD_DIM), BF16),
            pltpu.VMEM((ZL, planes, B, HEAD_DIM), BF16),
            pltpu.VMEM((B, 2, pad, HEAD_DIM), F32),
            pltpu.VMEM((GRP, 2, pad, HEAD_DIM), F32),
            dma((heads, 4)),
            dma((X, 2)), dma((B,)),
            dma((Z,)), dma((Z,)),
            dma((Y, Z)), dma((Y,)),
            dma((Y, Z)), dma((Y,)),
            dma((Y,)), dma((Y,)),
            dma((Y,)), dma((Y,)),
            dma((ZL,)), dma((ZL,)),
            dma((B,)), dma((GRP,)),
        ],
        compiler_params=pltpu.CompilerParams(collective_id=0, has_side_effects=True, vmem_limit_bytes=40 * 2**20),
        name="attention_tangent",
    )(queries, query_tangent, keys, key_tangent, values, value_tangent)


def solution(mesh):
    in_specs = (
        P(("grp", "seq"), None),
        P(("grp", "seq"), None),
        P("seq", "grp"),
        P("seq", "grp"),
        P("seq", "grp"),
        P("seq", "grp"),
    )
    out_specs = (P(("grp", "seq"), None), P(("grp", "seq"), None))
    return jax.shard_map(
        per_device, mesh=mesh, in_specs=in_specs, out_specs=out_specs, check_vma=False
    )
```
